512 devices in a mesh: lat: 16 (over x, z_lo, core), lon: 32 (over z_hi, y).
Axes of the slice: x: 4, y: 8, z: 8 (z_hi: 4, z_lo: 2; z = z_hi * 2 + z_lo), core: 2. Of those that a mesh axis runs over, the one named last changes fastest.
Arguments:
- tokens: bfloat16 [4, 224, 128, 1536], P(None, 'lat', 'lon'), may hold values from -400 to 400, as said below
- in_bounds: int32 [17], replicated, may hold values from 0 to 191, as said below
- out_bounds: int32 [17], replicated, may hold values from 0 to 96, as said below
- down_gain: float32 [768], replicated, may hold values from 0.25 to 1.75
- down_bias: float32 [768], replicated, may hold values from -1 to 1
- down_weight: bfloat16 [768, 384], replicated, may hold values from -0.21875 to 0.21875
- up_weight: bfloat16 [384, 768], replicated, may hold values from -0.3125 to 0.3125
- up_gain: float32 [192], replicated, may hold values from 0.25 to 1.75
- up_bias: float32 [192], replicated, may hold values from -1 to 1
- out_weight: bfloat16 [192, 192], replicated, may hold values from -0.4375 to 0.4375
Outputs:
- merged: bfloat16 [4, 128, 64, 3072], P(None, 'lat', 'lon')
- upsampled: bfloat16 [4, 224, 128, 1536], P(None, 'lat', 'lon')
The draws below stay inside these ranges and needn't reach their ends.
Inputs may be any that keep to these rules, and one draw needn't show every extreme that they name: `tokens`: band b's fine rows stand in its slots from the first one on; slots past the band's count hold values that no output reads. in_bounds[0] = 0, in_bounds[16] = 191; each band has 10 to 14 fine rows, and some band has 14. out_bounds[0] = 0, out_bounds[16] = 96; each band has 4 to 8 merged rows, and some band has 8. For 0 < b < 16, 2 * out_bounds[b] - in_bounds[b] is 1 to 3, and 3 for some b; so merged band b covers fine rows from band b's first on to at most 3 rows past its last (fine row 191 counting as zeros), and band b's fine rows need merged rows from at most 2 rows before merged band b's first up to its last, 2 being reached.
All inputs are finite; a program needn't handle non-finite values.
Results may differ from the reference program's by a relative error of at most 0.0069.
Values may be sent and summed in bfloat16 or wider, within the bound.
A program may use at most 64 MiB of HBM per device.

```python
import math
import jax
import jax.numpy as jnp
from jax import lax

C = 192
LEV = 8
ROWS_DEV = 12
LON_DEV = 4
MEMBERS = 4
LCAP = 14
MCAP = 8
LAT = 191
MLAT = 96
LON = 128
N_LAT = 16
N_LON = 32


def pick_three(pattern, first, second, third):
    return jnp.where(pattern == 0, first, jnp.where(pattern == 1, second, third))


def bound_pair(key):
    base_key = jax.random.fold_in(key, 11)
    key_index, key_pattern, key_extra = jax.random.split(base_key, 3)
    places = jnp.arange(N_LAT + 1, dtype=jnp.int32)
    coarse_table = jnp.array([0, 1, 1, 1, 2], jnp.int32)
    fine_table = jnp.array([-1, -1, 0, 1, 1], jnp.int32)
    choose = jax.random.randint(key_index, (N_LAT + 1,), 0, 5).astype(jnp.int32)
    coarse_moves = jnp.take(coarse_table, choose)
    fine_moves = jnp.take(fine_table, choose)
    pattern = jax.random.randint(key_pattern, (), 0, 3).astype(jnp.int32)
    extra = jax.random.randint(key_extra, (), -1, 2).astype(jnp.int32)
    coarse_one = pick_three(pattern, 0, 2, coarse_moves[1])
    fine_one = pick_three(pattern, -1, 1, fine_moves[1])
    coarse_two = pick_three(pattern, 2, 0, 0)
    fine_two = pick_three(pattern, 1, -1, -1)
    coarse_three = pick_three(pattern, 1, jnp.where(extra > 0, 2, 1), 2)
    fine_three = pick_three(pattern, extra, 1, 1)
    coarse_moves = jnp.where(places == 1, coarse_one, jnp.where(places == 2, coarse_two, jnp.where(places == 3, coarse_three, coarse_moves)))
    fine_moves = jnp.where(places == 1, fine_one, jnp.where(places == 2, fine_two, jnp.where(places == 3, fine_three, fine_moves)))
    edges = (places == 0) | (places == N_LAT)
    fine_moves = jnp.where(edges, 0, fine_moves)
    coarse_moves = jnp.where(edges, 0, coarse_moves)
    fine_bounds = places * ROWS_DEV + fine_moves
    fine_bounds = jnp.where(places == N_LAT, N_LAT * ROWS_DEV - 1, fine_bounds)
    coarse_bounds = places * (ROWS_DEV // 2) + coarse_moves
    return (fine_bounds.astype(jnp.int32), coarse_bounds.astype(jnp.int32))


def draw_in_bounds(key, part):
    return bound_pair(key)[0]


def draw_out_bounds(key, part):
    return bound_pair(key)[1]


def draw_tokens(key, part):
    key_base, key_rows, key_chan = jax.random.split(jax.random.fold_in(key, 5), 3)
    shape = (MEMBERS, N_LAT * (ROWS_DEV + 2), LON_DEV * N_LON, LEV * C)
    row_scale = jnp.exp(jax.random.uniform(key_rows, (MEMBERS, N_LAT * (ROWS_DEV + 2), LON_DEV * N_LON, 1), jnp.float32, 0.0, math.log(10.0)))
    chan_scale = jnp.exp(jax.random.uniform(key_chan, (1, 1, 1, LEV * C), jnp.float32, 0.0, math.log(10.0)))
    values = jnp.clip(jax.random.normal(key_base, shape, jnp.float32), -4.0, 4.0)
    return (values * row_scale * chan_scale).astype(jnp.bfloat16)


def bell_draw(stream_key, shape, width, reach, kind=jnp.bfloat16):
    return jnp.clip(width * jax.random.normal(stream_key, shape, jnp.float32), -reach, reach).astype(kind)


def setup_inputs(seed: int = 0) -> dict:
    seeds = jax.random.split(jax.random.key(seed), 11)
    return {
        "tokens": draw_tokens(jax.random.fold_in(seeds[10], 71), 0),
        "in_bounds": draw_in_bounds(jax.random.fold_in(seeds[10], 71), 0),
        "out_bounds": draw_out_bounds(jax.random.fold_in(seeds[10], 71), 0),
        "down_gain": jnp.clip(1.0 + 0.15 * jax.random.normal(seeds[3], (4 * C,), jnp.float32), 0.25, 1.75),
        "down_bias": bell_draw(seeds[4], (4 * C,), 0.3, 1.0, jnp.float32),
        "down_weight": bell_draw(seeds[5], (4 * C, 2 * C), (4 * C) ** -0.5, 0.21875),
        "up_weight": bell_draw(seeds[6], (2 * C, 4 * C), (2 * C) ** -0.5, 0.3125),
        "up_gain": jnp.clip(1.0 + 0.15 * jax.random.normal(seeds[7], (C,), jnp.float32), 0.25, 1.75),
        "up_bias": bell_draw(seeds[8], (C,), 0.3, 1.0, jnp.float32),
        "out_weight": bell_draw(seeds[9], (C, C), C ** -0.5, 0.4375),
    }


def layer_norm(values, scale_vec, shift_vec):
    center = lax.optimization_barrier(jnp.mean(values, axis=-1, keepdims=True))
    spread = lax.optimization_barrier(jnp.mean(jnp.square(values - center), axis=-1, keepdims=True))
    return (values - center) * lax.rsqrt(spread + 1e-05) * scale_vec + shift_vec

def reference(tokens, in_bounds, out_bounds, down_gain, down_bias, down_weight, up_weight, up_gain, up_bias, out_weight):
    half_lon = LON // 2
    lat_rows = jnp.arange(LAT, dtype=jnp.int32)
    band_of = lax.optimization_barrier(jnp.sum((lat_rows[:, None] >= in_bounds[None, 1:N_LAT]).astype(jnp.int32), axis=1)).astype(jnp.int32)
    slot_of = (band_of * LCAP + lat_rows - in_bounds[band_of]).astype(jnp.int32)

    def one_member(member):
        token_grid = jnp.take(member, slot_of, axis=0)
        token_grid = jnp.concatenate([token_grid, jnp.zeros((1, LON, LEV * C), jnp.bfloat16)], axis=0)
        token_grid = jnp.roll(token_grid, 1, axis=1)
        pieces = token_grid.reshape(MLAT, 2, half_lon, 2, LEV, C).transpose(0, 2, 4, 3, 1, 5).reshape(-1, 4 * C)
        normed = layer_norm(pieces.astype(jnp.float32), down_gain, down_bias).astype(jnp.bfloat16)
        coarse = jnp.dot(normed, down_weight, preferred_element_type=jnp.float32).astype(jnp.bfloat16)
        widened = jnp.dot(coarse, up_weight, preferred_element_type=jnp.float32).astype(jnp.bfloat16)
        widened = widened.reshape(MLAT, half_lon, LEV, 2, 2, C).transpose(0, 4, 1, 3, 2, 5).reshape(2 * MLAT, LON, LEV, C)
        widened = jnp.roll(widened, -1, axis=1)[:LAT]
        renormed = layer_norm(widened.astype(jnp.float32), up_gain, up_bias).astype(jnp.bfloat16)
        finished = jnp.dot(renormed.reshape(-1, C), out_weight, preferred_element_type=jnp.float32).astype(jnp.bfloat16)
        return (coarse.reshape(MLAT, half_lon, LEV * 2 * C), finished.reshape(LAT, LON, LEV * C))
    coarse_all, fine_all = lax.map(one_member, tokens)
    fine_slots = jnp.arange(N_LAT * LCAP, dtype=jnp.int32)
    fine_band = (fine_slots // LCAP).astype(jnp.int32)
    fine_offset = (fine_slots % LCAP).astype(jnp.int32)
    fine_source = jnp.clip(in_bounds[fine_band] + fine_offset, 0, LAT - 1).astype(jnp.int32)
    fine_live = fine_offset < in_bounds[fine_band + 1] - in_bounds[fine_band]
    upsampled = jnp.where(fine_live[None, :, None, None], jnp.take(fine_all, fine_source, axis=1), jnp.zeros((), jnp.bfloat16))
    coarse_slots = jnp.arange(N_LAT * MCAP, dtype=jnp.int32)
    coarse_band = (coarse_slots // MCAP).astype(jnp.int32)
    coarse_offset = (coarse_slots % MCAP).astype(jnp.int32)
    coarse_source = jnp.clip(out_bounds[coarse_band] + coarse_offset, 0, MLAT - 1).astype(jnp.int32)
    coarse_live = coarse_offset < out_bounds[coarse_band + 1] - out_bounds[coarse_band]
    merged = jnp.where(coarse_live[None, :, None, None], jnp.take(coarse_all, coarse_source, axis=1), jnp.zeros((), jnp.bfloat16))
    return (merged.astype(jnp.bfloat16), upsampled.astype(jnp.bfloat16))
```

```python
import functools

import jax
import jax.numpy as jnp
from jax import lax
from jax.experimental import pallas as pl
from jax.experimental.pallas import tpu as pltpu
from jax.sharding import PartitionSpec as P

MESH = pl.DeviceIdType.MESH
BF = jnp.bfloat16
F32 = jnp.float32
C = 192
LEV = 8
PAIRS = LEV // 2
E = 4
ROWS = 14
MS = 9
MR = 112
XR = 240


def iota(shape, dim):
    return lax.broadcasted_iota(jnp.int32, shape, dim)


def one_hot(target, width):
    return jnp.where(iota((target.shape[0], width), 1) == target, 1.0, 0.0).astype(BF)


def dot(a, b):
    return jnp.dot(a, b, preferred_element_type=F32)


def pair_sums(v):
    low = iota((v.shape[0], 128), 1) < 64
    mid = v[:, 128:256]
    even = v[:, 0:128] + jnp.where(low, mid, 0.0)
    odd = v[:, 256:384] + jnp.where(low, 0.0, mid)
    return jnp.sum(even, axis=1, keepdims=True), jnp.sum(odd, axis=1, keepdims=True)


def pair_lanes(even, odd, rows):
    low = iota((rows, 128), 1) < 64
    e = jnp.broadcast_to(even, (rows, 128))
    o = jnp.broadcast_to(odd, (rows, 128))
    return jnp.concatenate([e, jnp.where(low, e, o), o], axis=1)


def kernel(
    n_lat,
    n_lon,
    tok,
    inb,
    outb,
    dgain,
    dbias,
    dw,
    uw,
    ugain,
    ubias,
    ow,
    merged,
    ups,
    xs,
    hb,
    ha,
    sb,
    sa,
    g,
    ne,
    no,
    we,
    wo,
    ua,
    ub,
    uc,
    bd,
    co,
    yy,
    ee,
    rn,
    send_sem,
    recv_sem,
):
    lat = lax.axis_index("lat")
    lon = lax.axis_index("lon")
    north = lax.rem(lat + n_lat - 1, n_lat)
    south = lax.rem(lat + 1, n_lat)
    west = lax.rem(lon + n_lon - 1, n_lon)
    east = lax.rem(lon + 1, n_lon)
    around = [
        (north, west),
        (north, lon),
        (north, east),
        (lat, west),
        (lat, east),
        (south, west),
        (south, lon),
        (south, east),
    ]
    barrier = pltpu.get_barrier_semaphore()
    for where in around:
        pl.semaphore_signal(barrier, inc=1, device_id=where, device_id_type=MESH)

    start_in = inb[lat]
    count_in = inb[lat + 1] - start_in
    end_all = inb[n_lat]
    start_out = outb[lat]
    count_out = outb[lat + 1] - start_out
    start_m = start_in >> 1
    par = start_in & 1
    skip_m = start_out - start_m

    zero8 = jnp.zeros((8, LEV * C), BF)
    for x in (3, 0, 1, 2):
        col = x + 1
        j, c = col // 2, col % 2
        xs[c, j * 64 + 56 : j * 64 + 64, :] = zero8
        xs[c, j * 64 : j * 64 + 56, :] = tok[:, :, x, :].reshape(56, LEV * C)
    for x in range(4):
        sb[x] = tok[:, 0:3, x, :].reshape(12, LEV * C)
    for e in range(E):
        last = tok[e, jnp.clip(count_in - 1, 0, ROWS - 1)]
        for x in range(4):
            sa[x, e : e + 1, :] = last[x : x + 1, :]

    pl.semaphore_wait(barrier, 8)

    def send(k, src, dst, where):
        return pltpu.make_async_remote_copy(
            src_ref=src,
            dst_ref=dst,
            send_sem=send_sem.at[k],
            recv_sem=recv_sem.at[k],
            device_id=where,
            device_id_type=MESH,
        )

    copies = [
        send(0, xs.at[0, 128:192], xs.at[0, 0:64], (lat, east)),
        send(1, xs.at[1, 0:64], xs.at[1, 128:192], (lat, west)),
        send(2, sb, hb.at[1:5], (north, lon)),
        send(3, sa, ha.at[1:5], (south, lon)),
        send(4, sb.at[3], hb.at[0], (north, east)),
        send(5, sb.at[0], hb.at[5], (north, west)),
        send(6, sa.at[3], ha.at[0], (south, east)),
        send(7, sa.at[0], ha.at[5], (south, west)),
    ]
    for copy in copies:
        copy.start()

    for q in range(4):
        block = dw[q * C : (q + 1) * C, :]
        zero = jnp.zeros((64, 2 * C), BF)
        we[q * 256 : q * 256 + C, :] = block
        we[q * 256 + C : (q + 1) * 256, :] = zero
        wo[q * 256 : q * 256 + 64, :] = zero
        wo[q * 256 + 64 : (q + 1) * 256, :] = block
    zero64 = jnp.zeros((2 * C, 64), BF)
    for c in range(2):
        for a in range(2):
            q = c * 2 + a
            block = uw[:, q * C : (q + 1) * C]
            at = a * 128
            ua[c, :, at : at + 128] = block[:, 0:128]
            ub[c, 0 : 2 * C, at : at + 128] = jnp.concatenate([block[:, 128:192], zero64], axis=1)
            ub[c, 2 * C : 4 * C, at : at + 128] = jnp.concatenate([zero64, block[:, 0:64]], axis=1)
            uc[c, :, at : at + 128] = block[:, 64:192]
    zero_c = jnp.zeros((C, C), BF)
    small = ow[...]
    bd[0:C, :] = jnp.concatenate([small, zero_c], axis=1)
    bd[C : 2 * C, :] = jnp.concatenate([zero_c, small], axis=1)

    row = iota((MR, 1), 0)
    j = (row >= 36).astype(jnp.int32) + (row >= 72).astype(jnp.int32)
    rest = row - 36 * j
    m = rest >> 2
    e = rest & 3
    picks = []
    for a in range(2):
        off = 2 * m + a - par
        own = j * 64 + e * 14 + off
        below = 192 + j * 16 + e * 3 + (off - count_in)
        above = 192 + j * 16 + 12 + e
        is_own = (off >= 0) & (off < count_in)
        is_below = (off >= count_in) & (off < count_in + 3) & (start_in + off < end_all)
        target = jnp.where(is_own, own, jnp.where(is_below, below, jnp.where(off < 0, above, -1)))
        target = jnp.where(m < MS, target, -1)
        picks.append(one_hot(target, XR))

    for copy in copies:
        copy.wait()

    for col in range(6):
        j, c = col // 2, col % 2
        xs[c, 192 + j * 16 : 208 + j * 16, :] = jnp.concatenate([hb[col], ha[col]], axis=0)

    for c in range(2):
        for a in range(2):
            g[c * 2 + a] = dot(picks[a], xs[c]).astype(BF)

    gains = []
    for q in range(4):
        one_g = dgain[0:1, q * C : (q + 1) * C]
        one_b = dbias[0:1, q * C : (q + 1) * C]
        gains.append((jnp.concatenate([one_g, one_g], axis=1), jnp.concatenate([one_b, one_b], axis=1)))

    def norm_down(step, carry):
        rows = pl.ds(pl.multiple_of(step * 16, 16), 16)
        for lp in range(PAIRS):
            vals = [g[q, rows, lp * 384 : (lp + 1) * 384].astype(F32) for q in range(4)]
            even, odd = pair_sums((vals[0] + vals[1]) + (vals[2] + vals[3]))
            mean = pair_lanes(even * (1.0 / 768), odd * (1.0 / 768), 16)
            vals = [v - mean for v in vals]
            even, odd = pair_sums(
                (vals[0] * vals[0] + vals[1] * vals[1]) + (vals[2] * vals[2] + vals[3] * vals[3])
            )
            rstd = pair_lanes(
                lax.rsqrt(even * (1.0 / 768) + 1e-05), lax.rsqrt(odd * (1.0 / 768) + 1e-05), 16
            )
            at = pl.ds(pl.multiple_of(lp * MR + step * 16, 16), 16)
            for q in range(4):
                out = (vals[q] * rstd * gains[q][0] + gains[q][1]).astype(BF)
                ne[at, q * 256 : (q + 1) * 256] = out[:, 0:256]
                no[at, q * 256 : (q + 1) * 256] = out[:, 128:384]
        return carry

    lax.fori_loop(0, MR // 16, norm_down, 0)
    co[:, 0:384] = dot(ne[...], we[...]).astype(BF)
    co[:, 384:768] = dot(no[...], wo[...]).astype(BF)

    row = iota((64, 1), 0)
    e = row >> 4
    k = (row >> 1) & 7
    target = (row & 1) * 36 + (k + skip_m) * 4 + e
    pick = one_hot(jnp.where(k < count_out, target, -1), MR)
    for lp in range(PAIRS):
        part = dot(pick, co[lp * MR : (lp + 1) * MR, :]).astype(BF)
        merged[:, :, :, lp * 768 : (lp + 1) * 768] = part.reshape(E, 8, 2, 768)

    for c in range(2):
        for t in range(3):
            if t == 0:
                part = dot(co[:, 0:384], ua[c])
            elif t == 1:
                part = dot(co[...], ub[c])
            else:
                part = dot(co[:, 384:768], uc[c])
            part = part.astype(BF)
            for a in range(2):
                for lp in range(PAIRS):
                    yy[(c * 2 + a) * MR : (c * 2 + a + 1) * MR, lp * 384 + t * 128 : lp * 384 + (t + 1) * 128] = part[
                        lp * MR : (lp + 1) * MR, a * 128 : (a + 1) * 128
                    ]
    row = iota((224, 1), 0)
    e = (row >= 56).astype(jnp.int32) + (row >= 112).astype(jnp.int32) + (row >= 168).astype(jnp.int32)
    k = (row - 56 * e) >> 2
    x1 = (row & 3) + 1
    o = k + par
    target = ((x1 & 1) * 2 + (o & 1)) * MR + (x1 >> 1) * 36 + (o >> 1) * 4 + e
    live = k < count_in
    pick = one_hot(jnp.where(live, target, -1), 4 * MR)
    ee[...] = dot(pick, yy[...]).astype(BF)

    gain2 = jnp.concatenate([ugain[...], ugain[...]], axis=1)
    bias2 = jnp.concatenate([ubias[...], ubias[...]], axis=1)

    def norm_up(step, carry):
        rows = pl.ds(pl.multiple_of(step * 16, 16), 16)
        for lp in range(PAIRS):
            v = ee[rows, lp * 384 : (lp + 1) * 384].astype(F32)
            even, odd = pair_sums(v)
            v = v - pair_lanes(even * (1.0 / C), odd * (1.0 / C), 16)
            even, odd = pair_sums(v * v)
            rstd = pair_lanes(
                lax.rsqrt(even * (1.0 / C) + 1e-05), lax.rsqrt(odd * (1.0 / C) + 1e-05), 16
            )
            at = pl.ds(pl.multiple_of(lp * 224 + step * 16, 16), 16)
            rn[at, :] = (v * rstd * gain2 + bias2).astype(BF)
        return carry

    lax.fori_loop(0, 14, norm_up, 0)
    for lp in range(PAIRS):
        part = rn[lp * 224 : (lp + 1) * 224, :]
        left = dot(part, bd[:, 0:256])
        right = dot(part[:, 128:384], bd[128:384, 256:384])
        whole = jnp.where(live, jnp.concatenate([left, right], axis=1), 0.0).astype(BF)
        ups[:, :, :, lp * 384 : (lp + 1) * 384] = whole.reshape(E, ROWS, 4, 384)


def solution(mesh):
    n_lat, n_lon = mesh.shape["lat"], mesh.shape["lon"]
    vmem = pl.BlockSpec(memory_space=pltpu.VMEM)
    smem = pl.BlockSpec(memory_space=pltpu.SMEM)

    def body(tok, inb, outb, dgain, dbias, dw, uw, ugain, ubias, ow):
        wide = LEV * C
        return pl.pallas_call(
            functools.partial(kernel, n_lat, n_lon),
            out_shape=(
                jax.ShapeDtypeStruct((E, 8, 2, 2 * wide), BF),
                jax.ShapeDtypeStruct((E, ROWS, 4, wide), BF),
            ),
            in_specs=[vmem, smem, smem] + [vmem] * 7,
            out_specs=(vmem, vmem),
            scratch_shapes=[
                pltpu.VMEM((2, XR, wide), BF),
                pltpu.VMEM((6, 12, wide), BF),
                pltpu.VMEM((6, 4, wide), BF),
                pltpu.VMEM((4, 12, wide), BF),
                pltpu.VMEM((4, 4, wide), BF),
                pltpu.VMEM((4, MR, wide), BF),
                pltpu.VMEM((4 * MR, 1024), BF),
                pltpu.VMEM((4 * MR, 1024), BF),
                pltpu.VMEM((1024, 384), BF),
                pltpu.VMEM((1024, 384), BF),
                pltpu.VMEM((2, 384, 256), BF),
                pltpu.VMEM((2, 768, 256), BF),
                pltpu.VMEM((2, 384, 256), BF),
                pltpu.VMEM((384, 384), BF),
                pltpu.VMEM((4 * MR, 768), BF),
                pltpu.VMEM((4 * MR, wide), BF),
                pltpu.VMEM((224, wide), BF),
                pltpu.VMEM((4 * 224, 384), BF),
                pltpu.SemaphoreType.DMA((8,)),
                pltpu.SemaphoreType.DMA((8,)),
            ],
            compiler_params=pltpu.CompilerParams(
                collective_id=0, has_side_effects=True, vmem_limit_bytes=60000000
            ),
        )(
            tok,
            inb,
            outb,
            dgain.reshape(1, -1),
            dbias.reshape(1, -1),
            dw,
            uw,
            ugain.reshape(1, -1),
            ubias.reshape(1, -1),
            ow,
        )

    return jax.shard_map(
        body,
        mesh=mesh,
        in_specs=(P(None, "lat", "lon", None), P(), P(), P(), P(), P(), P(), P(), P(), P()),
        out_specs=(P(None, "lat", "lon", None), P(None, "lat", "lon", None)),
        check_vma=False,
    )
```

```python
import functools

import jax
import jax.numpy as jnp
from jax import lax
from jax.experimental import pallas as pl
from jax.experimental.pallas import tpu as pltpu
from jax.sharding import PartitionSpec as P

MESH = pl.DeviceIdType.MESH
BF = jnp.bfloat16
F32 = jnp.float32
C = 192
LEV = 8
PAIRS = LEV // 2
E = 4
ROWS = 14
MS = 9
AR = 80
SEND = 56
BR = 48


def iota(shape, dim):
    return lax.broadcasted_iota(jnp.int32, shape, dim)


def one_hot(target, width):
    return jnp.where(iota((target.shape[0], width), 1) == target, 1.0, 0.0).astype(BF)


def dot(a, b):
    return jnp.dot(a, b, preferred_element_type=F32)


def pair_sums(v):
    low = iota((v.shape[0], 128), 1) < 64
    mid = v[:, 128:256]
    even = v[:, 0:128] + jnp.where(low, mid, 0.0)
    odd = v[:, 256:384] + jnp.where(low, 0.0, mid)
    return jnp.sum(even, axis=1, keepdims=True), jnp.sum(odd, axis=1, keepdims=True)


def pair_lanes(even, odd, rows):
    low = iota((rows, 128), 1) < 64
    e = jnp.broadcast_to(even, (rows, 128))
    o = jnp.broadcast_to(odd, (rows, 128))
    return jnp.concatenate([e, jnp.where(low, e, o), o], axis=1)


def norm_rows(src, rows, ne, no, stack, gains, count):
    def step(i, carry):
        at = pl.ds(pl.multiple_of(i * 16, 16), 16)
        for lp in range(PAIRS):
            vals = [src[q, at, lp * 384 : (lp + 1) * 384].astype(F32) for q in range(4)]
            even, odd = pair_sums((vals[0] + vals[1]) + (vals[2] + vals[3]))
            mean = pair_lanes(even * (1.0 / 768), odd * (1.0 / 768), 16)
            vals = [v - mean for v in vals]
            even, odd = pair_sums(
                (vals[0] * vals[0] + vals[1] * vals[1]) + (vals[2] * vals[2] + vals[3] * vals[3])
            )
            rstd = pair_lanes(
                lax.rsqrt(even * (1.0 / 768) + 1e-05), lax.rsqrt(odd * (1.0 / 768) + 1e-05), 16
            )
            to = pl.ds(pl.multiple_of(lp * stack + i * 16, 16), 16)
            for q in range(4):
                out = (vals[q] * rstd * gains[q][0] + gains[q][1]).astype(BF)
                ne[to, q * 256 : (q + 1) * 256] = out[:, 0:256]
                no[to, q * 256 : (q + 1) * 256] = out[:, 128:384]
        return carry

    lax.fori_loop(0, count, step, 0)


def norm_fine(src, rn, stack, gain2, bias2, count):
    def step(i, carry):
        at = pl.ds(pl.multiple_of(i * 16, 16), 16)
        for lp in range(PAIRS):
            v = src[at, lp * 384 : (lp + 1) * 384].astype(F32)
            even, odd = pair_sums(v)
            v = v - pair_lanes(even * (1.0 / C), odd * (1.0 / C), 16)
            even, odd = pair_sums(v * v)
            rstd = pair_lanes(
                lax.rsqrt(even * (1.0 / C) + 1e-05), lax.rsqrt(odd * (1.0 / C) + 1e-05), 16
            )
            to = pl.ds(pl.multiple_of(lp * stack + i * 16, 16), 16)
            rn[to, :] = (v * rstd * gain2 + bias2).astype(BF)
        return carry

    lax.fori_loop(0, count, step, 0)


def expand(left, both, right, ua, ub, uc, c, yy, base, rows):
    for t in range(3):
        if t == 0:
            part = dot(left, ua[c])
        elif t == 1:
            part = dot(both, ub[c])
        else:
            part = dot(right, uc[c])
        part = part.astype(BF)
        for a in range(2):
            for lp in range(PAIRS):
                yy[base + a * rows : base + (a + 1) * rows, lp * 384 + t * 128 : lp * 384 + (t + 1) * 128] = part[
                    lp * rows : (lp + 1) * rows, a * 128 : (a + 1) * 128
                ]


def project(rn, stack, bd, fs, base, rows):
    left = dot(rn[...], bd[:, 0:256]).astype(BF)
    right = dot(rn[:, 128:384], bd[128:384, 256:384]).astype(BF)
    for lp in range(PAIRS):
        fs[base : base + rows, lp * 384 : lp * 384 + 256] = left[lp * stack : lp * stack + rows, :]
        fs[base : base + rows, lp * 384 + 256 : (lp + 1) * 384] = right[lp * stack : lp * stack + rows, :]


def kernel(
    n_lat,
    n_lon,
    tok_hbm,
    inb_hbm,
    outb_hbm,
    dgain_hbm,
    dbias_hbm,
    dw_hbm,
    uw_hbm,
    ugain_hbm,
    ubias_hbm,
    ow_hbm,
    merged,
    ups,
    inb,
    outb,
    dgain,
    dbias,
    ugain,
    ubias,
    tok,
    dw,
    uw,
    ow,
    xa,
    xb,
    sc,
    ew,
    ee,
    ls,
    ln,
    cws,
    cwn,
    ces,
    cen,
    ga,
    gb,
    nea,
    noa,
    neb,
    nob,
    we,
    wo,
    ua,
    ub,
    uc,
    bd,
    coa,
    cob,
    ya,
    yb,
    ea,
    eb,
    rna,
    rnb,
    fs,
    load_sem,
    send_sem,
    recv_sem,
):
    lat = lax.axis_index("lat")
    lon = lax.axis_index("lon")
    north = (lax.rem(lat + n_lat - 1, n_lat), lon)
    south = (lax.rem(lat + 1, n_lat), lon)
    west = (lat, lax.rem(lon + n_lon - 1, n_lon))
    east = (lat, lax.rem(lon + 1, n_lon))
    barrier = pltpu.get_barrier_semaphore()
    for where in (west, east, north, south):
        pl.semaphore_signal(barrier, inc=1, device_id=where, device_id_type=MESH)

    loads = [
        pltpu.make_async_copy(src, dst, load_sem.at[i])
        for i, (src, dst) in enumerate(
            (
                (inb_hbm, inb),
                (tok_hbm, tok),
                (outb_hbm, outb),
                (dgain_hbm, dgain),
                (dbias_hbm, dbias),
                (dw_hbm, dw),
                (uw_hbm, uw),
                (ugain_hbm, ugain),
                (ubias_hbm, ubias),
                (ow_hbm, ow),
            )
        )
    ]
    for load in loads:
        load.start()

    loads[0].wait()
    start_in = inb[lat]
    count_in = inb[lat + 1] - start_in
    end_all = inb[n_lat]
    start_m = start_in >> 1
    par = start_in & 1
    last_row = jnp.clip(count_in - 1, 0, ROWS - 1)

    def send(k, src, dst, where):
        return pltpu.make_async_remote_copy(
            src_ref=src,
            dst_ref=dst,
            send_sem=send_sem.at[k],
            recv_sem=recv_sem.at[k],
            device_id=where,
            device_id_type=MESH,
        )

    edge_east = send(0, sc.at[3], ew, east)
    main_east = send(1, xa.at[0, 64 : 64 + SEND], xb.at[0, 0:SEND], east)
    edge_west = send(2, sc.at[0], ee, west)
    main_west = send(3, xb.at[1, 0:SEND], xa.at[1, 64 : 64 + SEND], west)
    rows_north = send(4, sc, ls, north)
    rows_south = send(5, sc, ln, south)
    fwd_w_north = send(6, ew, cws, north)
    fwd_w_south = send(7, ew, cwn, south)
    fwd_e_north = send(8, ee, ces, north)
    fwd_e_south = send(9, ee, cen, south)

    zero8 = jnp.zeros((8, LEV * C), BF)

    def stage_edge(x):
        first = tok[:, 0:3, x, :].reshape(12, LEV * C)
        last = [tok[e, last_row][x : x + 1, :] for e in range(E)]
        sc[x] = jnp.concatenate([first] + last, axis=0)

    def stage_main(x, ref, c, at):
        ref[c, at : at + 56, :] = tok[:, :, x, :].reshape(56, LEV * C)
        ref[c, at + 56 : at + 64, :] = zero8

    loads[1].wait()
    stage_edge(3)
    stage_edge(0)
    stage_main(3, xa, 0, 64)
    stage_main(0, xb, 1, 0)
    pl.semaphore_wait(barrier, 4)
    edge_east.start()
    edge_west.start()
    main_east.start()
    main_west.start()
    stage_edge(1)
    stage_edge(2)
    rows_north.start()
    rows_south.start()
    stage_main(1, xa, 0, 0)
    stage_main(2, xa, 1, 0)
    xb[0, 56:64, :] = zero8
    xa[1, 120:128, :] = zero8

    for load in loads[2:]:
        load.wait()
    start_out = outb[lat]
    count_out = outb[lat + 1] - start_out
    skip_m = start_out - start_m
    for q in range(4):
        block = dw[q * C : (q + 1) * C, :]
        zero = jnp.zeros((64, 2 * C), BF)
        we[q * 256 : q * 256 + C, :] = block
        we[q * 256 + C : (q + 1) * 256, :] = zero
        wo[q * 256 : q * 256 + 64, :] = zero
        wo[q * 256 + 64 : (q + 1) * 256, :] = block
    zero64 = jnp.zeros((2 * C, 64), BF)
    for c in range(2):
        for a in range(2):
            q = c * 2 + a
            block = uw[:, q * C : (q + 1) * C]
            at = a * 128
            ua[c, :, at : at + 128] = block[:, 0:128]
            ub[c, 0 : 2 * C, at : at + 128] = jnp.concatenate([block[:, 128:192], zero64], axis=1)
            ub[c, 2 * C : 4 * C, at : at + 128] = jnp.concatenate([zero64, block[:, 0:64]], axis=1)
            uc[c, :, at : at + 128] = block[:, 64:192]
    zero_c = jnp.zeros((C, C), BF)
    small = ow[...]
    bd[0:C, :] = jnp.concatenate([small, zero_c], axis=1)
    bd[C : 2 * C, :] = jnp.concatenate([zero_c, small], axis=1)

    def row_pick(count, a, j, m, e):
        off = 2 * m + a - par
        own = j * 64 + e * 14 + off
        below = count * 64 + j * 16 + e * 3 + (off - count_in)
        above = count * 64 + j * 16 + 12 + e
        is_own = (off >= 0) & (off < count_in)
        is_below = (off >= count_in) & (off < count_in + 3) & (start_in + off < end_all)
        target = jnp.where(is_own, own, jnp.where(is_below, below, jnp.where(off < 0, above, -1)))
        return one_hot(jnp.where(m < MS, target, -1), count * 80)

    row = iota((AR, 1), 0)
    j = (row >= 36).astype(jnp.int32)
    rest = row - 36 * j
    picks_a = [row_pick(2, a, j, rest >> 2, rest & 3) for a in range(2)]
    row = iota((BR, 1), 0)
    picks_b = [row_pick(1, a, 0, row >> 2, row & 3) for a in range(2)]

    gains = []
    for q in range(4):
        one_g = dgain[...].reshape(1, 4 * C)[:, q * C : (q + 1) * C]
        one_b = dbias[...].reshape(1, 4 * C)[:, q * C : (q + 1) * C]
        gains.append((jnp.concatenate([one_g, one_g], axis=1), jnp.concatenate([one_b, one_b], axis=1)))
    one_g = ugain[...].reshape(1, C)
    one_b = ubias[...].reshape(1, C)
    gain2 = jnp.concatenate([one_g, one_g], axis=1)
    bias2 = jnp.concatenate([one_b, one_b], axis=1)

    tile_row = iota((16, LEV * C), 0)

    def halo(below, above):
        return jnp.where(tile_row < 12, below.astype(F32), above.astype(F32)).astype(BF)

    edge_west.wait_recv()
    fwd_e_north.start()
    fwd_e_south.start()
    edge_east.wait_recv()
    fwd_w_north.start()
    fwd_w_south.start()
    rows_north.wait_recv()
    rows_south.wait_recv()
    fwd_e_north.wait_recv()
    fwd_e_south.wait_recv()
    xa[0, 128:144, :] = halo(ls[1], ln[1])
    xa[0, 144:160, :] = halo(ls[3], ln[3])
    xa[1, 128:144, :] = halo(ls[2], ln[2])
    xa[1, 144:160, :] = halo(ces[...], cen[...])
    xb[1, 64:80, :] = halo(ls[0], ln[0])
    main_west.wait_recv()
    for c in range(2):
        for a in range(2):
            ga[c * 2 + a] = dot(picks_a[a], xa[c]).astype(BF)
    norm_rows(ga, AR, nea, noa, AR, gains, AR // 16)
    coa[:, 0:384] = dot(nea[...], we[...]).astype(BF)
    coa[:, 384:768] = dot(noa[...], wo[...]).astype(BF)
    expand(coa[:, 0:384], coa[...], coa[:, 384:768], ua, ub, uc, 0, ya, 0, AR)
    first = jnp.concatenate([coa[lp * AR : lp * AR + BR, :] for lp in range(PAIRS)], axis=0)
    expand(first[:, 0:384], first, first[:, 384:768], ua, ub, uc, 1, ya, 2 * AR, BR)
    row = iota((176, 1), 0)
    x = (row >= 56).astype(jnp.int32) + (row >= 112).astype(jnp.int32)
    rest = row - 56 * x
    e = (rest >= 14).astype(jnp.int32) + (rest >= 28).astype(jnp.int32) + (rest >= 42).astype(jnp.int32)
    o = rest - 14 * e + par
    spot = (o >> 1) * 4 + e
    target = jnp.where(x == 1, 2 * AR + (o & 1) * BR + spot, (o & 1) * AR + spot + (x >> 1) * 36)
    pick = one_hot(jnp.where(row < 168, target, -1), 2 * AR + 2 * BR)
    ea[...] = dot(pick, ya[...]).astype(BF)
    norm_fine(ea, rna, 176, gain2, bias2, 11)
    project(rna, 176, bd, fs, 64, 176)

    fwd_w_north.wait_recv()
    fwd_w_south.wait_recv()
    xb[0, 64:80, :] = halo(cws[...], cwn[...])
    row = iota((64, 1), 0)
    e = (row >= 14).astype(jnp.int32) + (row >= 28).astype(jnp.int32) + (row >= 42).astype(jnp.int32)
    o = row - 14 * e + par
    target = (o & 1) * BR + (o >> 1) * 4 + e
    pick_b = one_hot(jnp.where(row < 56, target, -1), 2 * BR)
    row = iota((224, 1), 0)
    e = (row >= 56).astype(jnp.int32) + (row >= 112).astype(jnp.int32) + (row >= 168).astype(jnp.int32)
    k = (row - 56 * e) >> 2
    x = row & 3
    target = e * 14 + k + jnp.where(x > 0, 8 + x * 56, 0)
    pick_fine = one_hot(jnp.where(k < count_in, target, -1), 240)
    row = iota((64, 1), 0)
    k = (row >> 1) & 7
    target = (k + skip_m) * 4 + (row >> 4)
    live = k < count_out
    pick_m0 = one_hot(jnp.where(live & ((row & 1) == 0), target, -1), BR)
    pick_m1 = one_hot(jnp.where(live & ((row & 1) == 1), target, -1), BR)

    main_east.wait_recv()
    for c in range(2):
        for a in range(2):
            gb[c * 2 + a] = dot(picks_b[a], xb[c]).astype(BF)
    norm_rows(gb, BR, neb, nob, BR, gains, BR // 16)
    cob[:, 0:384] = dot(neb[...], we[...]).astype(BF)
    cob[:, 384:768] = dot(nob[...], wo[...]).astype(BF)
    for lp in range(PAIRS):
        part = dot(pick_m0, cob[lp * BR : (lp + 1) * BR, :]) + dot(pick_m1, coa[lp * AR : lp * AR + BR, :])
        merged[:, :, :, lp * 768 : (lp + 1) * 768] = part.astype(BF).reshape(E, 8, 2, 768)
    expand(cob[:, 0:384], cob[...], cob[:, 384:768], ua, ub, uc, 1, yb, 0, BR)
    eb[...] = dot(pick_b, yb[...]).astype(BF)
    norm_fine(eb, rnb, 64, gain2, bias2, 4)
    project(rnb, 64, bd, fs, 0, 64)
    for lp in range(PAIRS):
        part = dot(pick_fine, fs[:, lp * 384 : (lp + 1) * 384]).astype(BF)
        ups[:, :, :, lp * 384 : (lp + 1) * 384] = part.reshape(E, ROWS, 4, 384)

    edge_east.wait_send()
    main_east.wait_send()
    edge_west.wait_send()
    main_west.wait_send()
    for copy in (rows_north, rows_south, fwd_w_north, fwd_w_south, fwd_e_north, fwd_e_south):
        copy.wait_send()


def copy_out(merged_in, ups_in, merged, ups, sem):
    first = pltpu.make_async_copy(merged_in, merged, sem.at[0])
    second = pltpu.make_async_copy(ups_in, ups, sem.at[1])
    first.start()
    second.start()
    first.wait()
    second.wait()


def solution(mesh):
    n_lat, n_lon = mesh.shape["lat"], mesh.shape["lon"]
    vmem = pl.BlockSpec(memory_space=pltpu.VMEM)
    hbm = pl.BlockSpec(memory_space=pltpu.HBM)
    wide = LEV * C
    outs = (
        jax.ShapeDtypeStruct((E, 8, 2, 2 * wide), BF),
        jax.ShapeDtypeStruct((E, ROWS, 4, wide), BF),
    )

    def body(tok, inb, outb, dgain, dbias, dw, uw, ugain, ubias, ow):
        held = pl.pallas_call(
            functools.partial(kernel, n_lat, n_lon),
            out_shape=outs,
            in_specs=[hbm] * 10,
            out_specs=(vmem, vmem),
            scratch_shapes=[
                pltpu.SMEM((n_lat + 1,), jnp.int32),
                pltpu.SMEM((n_lat + 1,), jnp.int32),
                pltpu.VMEM((4 * C,), F32),
                pltpu.VMEM((4 * C,), F32),
                pltpu.VMEM((C,), F32),
                pltpu.VMEM((C,), F32),
                pltpu.VMEM((E, ROWS, 4, wide), BF),
                pltpu.VMEM((4 * C, 2 * C), BF),
                pltpu.VMEM((2 * C, 4 * C), BF),
                pltpu.VMEM((C, C), BF),
                pltpu.VMEM((2, 160, wide), BF),
                pltpu.VMEM((2, 80, wide), BF),
                pltpu.VMEM((4, 16, wide), BF),
                pltpu.VMEM((16, wide), BF),
                pltpu.VMEM((16, wide), BF),
                pltpu.VMEM((4, 16, wide), BF),
                pltpu.VMEM((4, 16, wide), BF),
                pltpu.VMEM((16, wide), BF),
                pltpu.VMEM((16, wide), BF),
                pltpu.VMEM((16, wide), BF),
                pltpu.VMEM((16, wide), BF),
                pltpu.VMEM((4, AR, wide), BF),
                pltpu.VMEM((4, BR, wide), BF),
                pltpu.VMEM((4 * AR, 1024), BF),
                pltpu.VMEM((4 * AR, 1024), BF),
                pltpu.VMEM((4 * BR, 1024), BF),
                pltpu.VMEM((4 * BR, 1024), BF),
                pltpu.VMEM((1024, 384), BF),
                pltpu.VMEM((1024, 384), BF),
                pltpu.VMEM((2, 384, 256), BF),
                pltpu.VMEM((2, 768, 256), BF),
                pltpu.VMEM((2, 384, 256), BF),
                pltpu.VMEM((384, 384), BF),
                pltpu.VMEM((4 * AR, 768), BF),
                pltpu.VMEM((4 * BR, 768), BF),
                pltpu.VMEM((2 * AR + 2 * BR, wide), BF),
                pltpu.VMEM((2 * BR, wide), BF),
                pltpu.VMEM((176, wide), BF),
                pltpu.VMEM((64, wide), BF),
                pltpu.VMEM((4 * 176, 384), BF),
                pltpu.VMEM((4 * 64, 384), BF),
                pltpu.VMEM((240, wide), BF),
                pltpu.SemaphoreType.DMA((10,)),
                pltpu.SemaphoreType.DMA((10,)),
                pltpu.SemaphoreType.DMA((10,)),
            ],
            compiler_params=pltpu.CompilerParams(
                collective_id=0, has_side_effects=True, vmem_limit_bytes=40000000
            ),
        )(*[pltpu.with_memory_space_constraint(v, pltpu.HBM) for v in (tok, inb, outb, dgain, dbias, dw, uw, ugain, ubias, ow)])
        return pl.pallas_call(
            copy_out,
            out_shape=outs,
            in_specs=[vmem, vmem],
            out_specs=(hbm, hbm),
            scratch_shapes=[pltpu.SemaphoreType.DMA((2,))],
            compiler_params=pltpu.CompilerParams(vmem_limit_bytes=4000000),
        )(*held)

    return jax.shard_map(
        body,
        mesh=mesh,
        in_specs=(P(None, "lat", "lon", None), P(), P(), P(), P(), P(), P(), P(), P(), P()),
        out_specs=(P(None, "lat", "lon", None), P(None, "lat", "lon", None)),
        check_vma=False,
    )
```

```python
import functools

import jax
import jax.numpy as jnp
from jax import lax
from jax.experimental import pallas as pl
from jax.experimental.pallas import tpu as pltpu
from jax.sharding import PartitionSpec as P

MESH = pl.DeviceIdType.MESH
BF = jnp.bfloat16
F32 = jnp.float32
C = 192
LEV = 8
PAIRS = LEV // 2
E = 4
ROWS = 14
MS = 9
AR = 80
SEND = 56
CUTS = (0, 16, 32, 48, 56)
PIECES = len(CUTS) - 1
BR = 48


def iota(shape, dim):
    return lax.broadcasted_iota(jnp.int32, shape, dim)


def one_hot(target, width):
    return jnp.where(iota((target.shape[0], width), 1) == target, 1.0, 0.0).astype(BF)


def dot(a, b):
    return jnp.dot(a, b, preferred_element_type=F32)


def pair_sums(v):
    low = iota((v.shape[0], 128), 1) < 64
    mid = v[:, 128:256]
    even = v[:, 0:128] + jnp.where(low, mid, 0.0)
    odd = v[:, 256:384] + jnp.where(low, 0.0, mid)
    return jnp.sum(even, axis=1, keepdims=True), jnp.sum(odd, axis=1, keepdims=True)


def pair_lanes(even, odd, rows):
    low = iota((rows, 128), 1) < 64
    e = jnp.broadcast_to(even, (rows, 128))
    o = jnp.broadcast_to(odd, (rows, 128))
    return jnp.concatenate([e, jnp.where(low, e, o), o], axis=1)


def norm_rows(src, rows, ne, no, stack, gains, count):
    def step(i, carry):
        at = pl.ds(pl.multiple_of(i * 16, 16), 16)
        for lp in range(PAIRS):
            vals = [src[q, at, lp * 384 : (lp + 1) * 384].astype(F32) for q in range(4)]
            even, odd = pair_sums((vals[0] + vals[1]) + (vals[2] + vals[3]))
            mean = pair_lanes(even * (1.0 / 768), odd * (1.0 / 768), 16)
            vals = [v - mean for v in vals]
            even, odd = pair_sums(
                (vals[0] * vals[0] + vals[1] * vals[1]) + (vals[2] * vals[2] + vals[3] * vals[3])
            )
            rstd = pair_lanes(
                lax.rsqrt(even * (1.0 / 768) + 1e-05), lax.rsqrt(odd * (1.0 / 768) + 1e-05), 16
            )
            to = pl.ds(pl.multiple_of(lp * stack + i * 16, 16), 16)
            for q in range(4):
                out = (vals[q] * rstd * gains[q][0] + gains[q][1]).astype(BF)
                ne[to, q * 256 : (q + 1) * 256] = out[:, 0:256]
                no[to, q * 256 : (q + 1) * 256] = out[:, 128:384]
        return carry

    lax.fori_loop(0, count, step, 0)


def norm_fine(src, rn, stack, gain2, bias2, count):
    def step(i, carry):
        at = pl.ds(pl.multiple_of(i * 16, 16), 16)
        for lp in range(PAIRS):
            v = src[at, lp * 384 : (lp + 1) * 384].astype(F32)
            even, odd = pair_sums(v)
            v = v - pair_lanes(even * (1.0 / C), odd * (1.0 / C), 16)
            even, odd = pair_sums(v * v)
            rstd = pair_lanes(
                lax.rsqrt(even * (1.0 / C) + 1e-05), lax.rsqrt(odd * (1.0 / C) + 1e-05), 16
            )
            to = pl.ds(pl.multiple_of(lp * stack + i * 16, 16), 16)
            rn[to, :] = (v * rstd * gain2 + bias2).astype(BF)
        return carry

    lax.fori_loop(0, count, step, 0)


def expand(left, both, right, ua, ub, uc, c, yy, base, rows):
    for t in range(3):
        if t == 0:
            part = dot(left, ua[c])
        elif t == 1:
            part = dot(both, ub[c])
        else:
            part = dot(right, uc[c])
        part = part.astype(BF)
        for a in range(2):
            for lp in range(PAIRS):
                yy[base + a * rows : base + (a + 1) * rows, lp * 384 + t * 128 : lp * 384 + (t + 1) * 128] = part[
                    lp * rows : (lp + 1) * rows, a * 128 : (a + 1) * 128
                ]


def project(rn, stack, bd, fs, base, rows):
    left = dot(rn[...], bd[:, 0:256]).astype(BF)
    right = dot(rn[:, 128:384], bd[128:384, 256:384]).astype(BF)
    for lp in range(PAIRS):
        fs[base : base + rows, lp * 384 : lp * 384 + 256] = left[lp * stack : lp * stack + rows, :]
        fs[base : base + rows, lp * 384 + 256 : (lp + 1) * 384] = right[lp * stack : lp * stack + rows, :]


def kernel(
    n_lat,
    n_lon,
    tok_hbm,
    inb_hbm,
    outb_hbm,
    dgain_hbm,
    dbias_hbm,
    dw_hbm,
    uw_hbm,
    ugain_hbm,
    ubias_hbm,
    ow_hbm,
    merged,
    ups,
    inb,
    outb,
    dgain,
    dbias,
    ugain,
    ubias,
    tok,
    dw,
    uw,
    ow,
    xa,
    xb,
    sc,
    ls,
    ln,
    cws,
    cwn,
    ces,
    cen,
    ga,
    gb,
    nea,
    noa,
    neb,
    nob,
    we,
    wo,
    ua,
    ub,
    uc,
    bd,
    coa,
    cob,
    ya,
    yb,
    ea,
    eb,
    rna,
    rnb,
    fs,
    relay,
    ready,
    load_sem,
    send_sem,
    recv_sem,
):
    lat = lax.axis_index("lat")
    lon = lax.axis_index("lon")
    north = (lax.rem(lat + n_lat - 1, n_lat), lon)
    south = (lax.rem(lat + 1, n_lat), lon)
    west = (lat, lax.rem(lon + n_lon - 1, n_lon))
    east = (lat, lax.rem(lon + 1, n_lon))
    n_west, n_east = (north[0], west[1]), (north[0], east[1])
    s_west, s_east = (south[0], west[1]), (south[0], east[1])
    barrier = pltpu.get_barrier_semaphore()
    has_n = lat > 0
    has_s = lat < n_lat - 1
    y = lax.rem(lon, 8)
    relays = n_lon % 8 == 0 and n_lon > 8 and n_lat % 4 == 0
    odd = lax.rem(lat // 2, 2) == 1
    role_7 = odd & (y == 7)
    role_0 = odd & (y == 0)
    far_up = (lat, lax.rem(lon + 8, n_lon))
    far_down = (lat, lax.rem(lon + n_lon - 8, n_lon))
    pair_up = (lat, lax.rem(lon + 7, n_lon))
    pair_down = (lat, lax.rem(lon + n_lon - 7, n_lon))

    def tell(where):
        pl.semaphore_signal(barrier, inc=1, device_id=where, device_id_type=MESH)

    def both(first, second):
        def run():
            first()
            second()

        return run

    tell(west)
    pl.when(has_n)(both(lambda: tell(north), lambda: tell(n_west)))
    pl.when(has_s)(both(lambda: tell(south), lambda: tell(s_west)))
    if relays:
        pl.when(role_7)(both(lambda: tell(far_down), lambda: tell(pair_down)))
        pl.when(role_0)(both(lambda: tell(far_up), lambda: tell(pair_up)))

    loads = [
        pltpu.make_async_copy(src, dst, load_sem.at[i])
        for i, (src, dst) in enumerate(
            (
                (inb_hbm, inb),
                (tok_hbm, tok),
                (outb_hbm, outb),
                (dgain_hbm, dgain),
                (dbias_hbm, dbias),
                (dw_hbm, dw),
                (uw_hbm, uw),
                (ugain_hbm, ugain),
                (ubias_hbm, ubias),
                (ow_hbm, ow),
            )
        )
    ]
    for load in loads:
        load.start()

    loads[0].wait()
    start_in = inb[lat]
    count_in = inb[lat + 1] - start_in
    end_all = inb[n_lat]
    start_m = start_in >> 1
    par = start_in & 1
    last_row = jnp.clip(count_in - 1, 0, ROWS - 1)

    def send(k, src, dst, where):
        return pltpu.make_async_remote_copy(
            src_ref=src,
            dst_ref=dst,
            send_sem=send_sem.at[k],
            recv_sem=recv_sem.at[k],
            device_id=where,
            device_id_type=MESH,
        )

    main_east = send(1, xa.at[0, 64 : 64 + SEND], xb.at[0, 0:SEND], east)
    main_west = send(3, xb.at[1, 0:SEND], xa.at[1, 64 : 64 + SEND], west)
    rows_north = send(4, sc, ls, north)
    rows_south = send(5, sc.at[:, 8:16], ln.at[:, 8:16], south)
    to_ne = send(6, sc.at[3], cws, n_east)
    to_se = send(7, sc.at[3, 8:16], cwn.at[8:16], s_east)
    to_nw = send(8, sc.at[0], ces, n_west)
    to_sw = send(9, sc.at[0, 8:16], cen.at[8:16], s_west)

    up_7, up_0, on_7, on_0 = [], [], [], []
    for i in range(PIECES):
        r0, r1 = CUTS[i], CUTS[i + 1]
        held = relay.at[r0:r1]
        up_7.append(send(10 + i, xa.at[0, 64 + r0 : 64 + r1], held, far_up))
        up_0.append(send(10 + i, xb.at[1, r0:r1], held, far_down))
        on_7.append(send(10 + PIECES + i, held, xb.at[0, r0:r1], pair_down))
        on_0.append(send(10 + PIECES + i, held, xa.at[1, 64 + r0 : 64 + r1], pair_up))

    zero8 = jnp.zeros((8, LEV * C), BF)

    def no_north():
        ln[...] = jnp.zeros_like(ln)
        cwn[...] = jnp.zeros_like(cwn)
        cen[...] = jnp.zeros_like(cen)

    def no_south():
        ls[...] = jnp.zeros_like(ls)
        cws[...] = jnp.zeros_like(cws)
        ces[...] = jnp.zeros_like(ces)

    pl.when(jnp.logical_not(has_n))(no_north)
    pl.when(jnp.logical_not(has_s))(no_south)

    def stage_edge(x):
        first = tok[:, 0:3, x, :].reshape(12, LEV * C)
        last = [tok[e, last_row][x : x + 1, :] for e in range(E)]
        sc[x] = jnp.concatenate([first] + last, axis=0)

    def stage_main(x, ref, c, at):
        ref[c, at : at + 56, :] = tok[:, :, x, :].reshape(56, LEV * C)
        ref[c, at + 56 : at + 64, :] = zero8

    arrivals = 1 + 2 * has_n.astype(jnp.int32) + 2 * has_s.astype(jnp.int32)
    if relays:
        arrivals = arrivals + 2 * (role_7 | role_0).astype(jnp.int32)
    pl.semaphore_wait(barrier, arrivals)

    def tell_ready(where):
        pl.semaphore_signal(ready, inc=1, device_id=where, device_id_type=MESH)

    tell_ready(east)
    pl.when(has_n)(lambda: tell_ready(n_east))
    pl.when(has_s)(lambda: tell_ready(s_east))
    loads[1].wait()
    for x in (3, 0, 1, 2):
        stage_edge(x)
    stage_main(3, xa, 0, 64)
    stage_main(0, xb, 1, 0)
    pl.when(has_n)(rows_north.start)
    pl.when(has_s)(rows_south.start)
    pl.when(has_n)(to_ne.start)
    pl.when(has_s)(to_se.start)
    if relays:
        pl.when(jnp.logical_not(role_7))(main_east.start)
        for i in range(PIECES):
            pl.when(role_7)(up_7[i].start)
    else:
        main_east.start()
    pl.semaphore_wait(ready, 1 + has_n.astype(jnp.int32) + has_s.astype(jnp.int32))
    pl.when(has_n)(to_nw.start)
    pl.when(has_s)(to_sw.start)
    if relays:
        pl.when(jnp.logical_not(role_0))(main_west.start)
        for i in range(PIECES):
            pl.when(role_0)(up_0[i].start)
    else:
        main_west.start()
    stage_main(1, xa, 0, 0)
    stage_main(2, xa, 1, 0)
    xb[0, 56:64, :] = zero8
    xa[1, 120:128, :] = zero8

    for load in loads[2:]:
        load.wait()
    start_out = outb[lat]
    count_out = outb[lat + 1] - start_out
    skip_m = start_out - start_m
    for q in range(4):
        block = dw[q * C : (q + 1) * C, :]
        zero = jnp.zeros((64, 2 * C), BF)
        we[q * 256 : q * 256 + C, :] = block
        we[q * 256 + C : (q + 1) * 256, :] = zero
        wo[q * 256 : q * 256 + 64, :] = zero
        wo[q * 256 + 64 : (q + 1) * 256, :] = block
    zero64 = jnp.zeros((2 * C, 64), BF)
    for c in range(2):
        for a in range(2):
            q = c * 2 + a
            block = uw[:, q * C : (q + 1) * C]
            at = a * 128
            ua[c, :, at : at + 128] = block[:, 0:128]
            ub[c, 0 : 2 * C, at : at + 128] = jnp.concatenate([block[:, 128:192], zero64], axis=1)
            ub[c, 2 * C : 4 * C, at : at + 128] = jnp.concatenate([zero64, block[:, 0:64]], axis=1)
            uc[c, :, at : at + 128] = block[:, 64:192]
    zero_c = jnp.zeros((C, C), BF)
    small = ow[...]
    bd[0:C, :] = jnp.concatenate([small, zero_c], axis=1)
    bd[C : 2 * C, :] = jnp.concatenate([zero_c, small], axis=1)

    def row_pick(count, a, j, m, e):
        off = 2 * m + a - par
        own = j * 64 + e * 14 + off
        below = count * 64 + j * 16 + e * 3 + (off - count_in)
        above = count * 64 + j * 16 + 12 + e
        is_own = (off >= 0) & (off < count_in)
        is_below = (off >= count_in) & (off < count_in + 3) & (start_in + off < end_all)
        target = jnp.where(is_own, own, jnp.where(is_below, below, jnp.where(off < 0, above, -1)))
        return one_hot(jnp.where(m < MS, target, -1), count * 80)

    row = iota((AR, 1), 0)
    j = (row >= 36).astype(jnp.int32)
    rest = row - 36 * j
    picks_a = [row_pick(2, a, j, rest >> 2, rest & 3) for a in range(2)]
    row = iota((BR, 1), 0)
    picks_b = [row_pick(1, a, 0, row >> 2, row & 3) for a in range(2)]

    gains = []
    for q in range(4):
        one_g = dgain[...].reshape(1, 4 * C)[:, q * C : (q + 1) * C]
        one_b = dbias[...].reshape(1, 4 * C)[:, q * C : (q + 1) * C]
        gains.append((jnp.concatenate([one_g, one_g], axis=1), jnp.concatenate([one_b, one_b], axis=1)))
    one_g = ugain[...].reshape(1, C)
    one_b = ubias[...].reshape(1, C)
    gain2 = jnp.concatenate([one_g, one_g], axis=1)
    bias2 = jnp.concatenate([one_b, one_b], axis=1)

    tile_row = iota((16, LEV * C), 0)

    def halo(below, above):
        return jnp.where(tile_row < 12, below.astype(F32), above.astype(F32)).astype(BF)

    if relays:
        for i in range(PIECES):
            pl.when(role_7)(both(up_7[i].wait_recv, on_7[i].start))
            pl.when(role_0)(both(up_0[i].wait_recv, on_0[i].start))
    pl.when(has_s)(both(rows_north.wait_recv, to_nw.wait_recv))
    pl.when(has_n)(both(rows_south.wait_recv, to_sw.wait_recv))
    xa[0, 128:144, :] = halo(ls[1], ln[1])
    xa[0, 144:160, :] = halo(ls[3], ln[3])
    xa[1, 128:144, :] = halo(ls[2], ln[2])
    xa[1, 144:160, :] = halo(ces[...], cen[...])
    xb[1, 64:80, :] = halo(ls[0], ln[0])
    if relays:
        pl.when(jnp.logical_not(role_7))(main_west.wait_recv)
        for i in range(PIECES):
            pl.when(role_7)(on_0[i].wait_recv)
    else:
        main_west.wait_recv()
    for c in range(2):
        for a in range(2):
            ga[c * 2 + a] = dot(picks_a[a], xa[c]).astype(BF)
    norm_rows(ga, AR, nea, noa, AR, gains, AR // 16)
    coa[:, 0:384] = dot(nea[...], we[...]).astype(BF)
    coa[:, 384:768] = dot(noa[...], wo[...]).astype(BF)
    expand(coa[:, 0:384], coa[...], coa[:, 384:768], ua, ub, uc, 0, ya, 0, AR)
    first = jnp.concatenate([coa[lp * AR : lp * AR + BR, :] for lp in range(PAIRS)], axis=0)
    expand(first[:, 0:384], first, first[:, 384:768], ua, ub, uc, 1, ya, 2 * AR, BR)
    row = iota((176, 1), 0)
    x = (row >= 56).astype(jnp.int32) + (row >= 112).astype(jnp.int32)
    rest = row - 56 * x
    e = (rest >= 14).astype(jnp.int32) + (rest >= 28).astype(jnp.int32) + (rest >= 42).astype(jnp.int32)
    o = rest - 14 * e + par
    spot = (o >> 1) * 4 + e
    target = jnp.where(x == 1, 2 * AR + (o & 1) * BR + spot, (o & 1) * AR + spot + (x >> 1) * 36)
    pick = one_hot(jnp.where(row < 168, target, -1), 2 * AR + 2 * BR)
    ea[...] = dot(pick, ya[...]).astype(BF)
    norm_fine(ea, rna, 176, gain2, bias2, 11)
    project(rna, 176, bd, fs, 64, 176)

    pl.when(has_s)(to_ne.wait_recv)
    pl.when(has_n)(to_se.wait_recv)
    xb[0, 64:80, :] = halo(cws[...], cwn[...])
    row = iota((64, 1), 0)
    e = (row >= 14).astype(jnp.int32) + (row >= 28).astype(jnp.int32) + (row >= 42).astype(jnp.int32)
    o = row - 14 * e + par
    target = (o & 1) * BR + (o >> 1) * 4 + e
    pick_b = one_hot(jnp.where(row < 56, target, -1), 2 * BR)
    row = iota((224, 1), 0)
    e = (row >= 56).astype(jnp.int32) + (row >= 112).astype(jnp.int32) + (row >= 168).astype(jnp.int32)
    k = (row - 56 * e) >> 2
    x = row & 3
    target = e * 14 + k + jnp.where(x > 0, 8 + x * 56, 0)
    pick_fine = one_hot(jnp.where(k < count_in, target, -1), 240)
    row = iota((64, 1), 0)
    k = (row >> 1) & 7
    target = (k + skip_m) * 4 + (row >> 4)
    live = k < count_out
    pick_m0 = one_hot(jnp.where(live & ((row & 1) == 0), target, -1), BR)
    pick_m1 = one_hot(jnp.where(live & ((row & 1) == 1), target, -1), BR)

    if relays:
        pl.when(jnp.logical_not(role_0))(main_east.wait_recv)
        for i in range(PIECES):
            pl.when(role_0)(on_7[i].wait_recv)
    else:
        main_east.wait_recv()
    for c in range(2):
        for a in range(2):
            gb[c * 2 + a] = dot(picks_b[a], xb[c]).astype(BF)
    norm_rows(gb, BR, neb, nob, BR, gains, BR // 16)
    cob[:, 0:384] = dot(neb[...], we[...]).astype(BF)
    cob[:, 384:768] = dot(nob[...], wo[...]).astype(BF)
    for lp in range(PAIRS):
        part = dot(pick_m0, cob[lp * BR : (lp + 1) * BR, :]) + dot(pick_m1, coa[lp * AR : lp * AR + BR, :])
        merged[:, :, :, lp * 768 : (lp + 1) * 768] = part.astype(BF).reshape(E, 8, 2, 768)
    expand(cob[:, 0:384], cob[...], cob[:, 384:768], ua, ub, uc, 1, yb, 0, BR)
    eb[...] = dot(pick_b, yb[...]).astype(BF)
    norm_fine(eb, rnb, 64, gain2, bias2, 4)
    project(rnb, 64, bd, fs, 0, 64)
    for lp in range(PAIRS):
        part = dot(pick_fine, fs[:, lp * 384 : (lp + 1) * 384]).astype(BF)
        ups[:, :, :, lp * 384 : (lp + 1) * 384] = part.reshape(E, ROWS, 4, 384)

    if relays:
        pl.when(jnp.logical_not(role_7))(main_east.wait_send)
        pl.when(jnp.logical_not(role_0))(main_west.wait_send)
        for i in range(PIECES):
            pl.when(role_7)(both(up_7[i].wait_send, on_7[i].wait_send))
            pl.when(role_0)(both(up_0[i].wait_send, on_0[i].wait_send))
    else:
        main_east.wait_send()
        main_west.wait_send()
    for copy in (rows_north, to_ne, to_nw):
        pl.when(has_n)(copy.wait_send)
    for copy in (rows_south, to_se, to_sw):
        pl.when(has_s)(copy.wait_send)


def copy_out(merged_in, ups_in, merged, ups, sem):
    first = pltpu.make_async_copy(merged_in, merged, sem.at[0])
    second = pltpu.make_async_copy(ups_in, ups, sem.at[1])
    first.start()
    second.start()
    first.wait()
    second.wait()


def solution(mesh):
    n_lat, n_lon = mesh.shape["lat"], mesh.shape["lon"]
    vmem = pl.BlockSpec(memory_space=pltpu.VMEM)
    hbm = pl.BlockSpec(memory_space=pltpu.HBM)
    wide = LEV * C
    outs = (
        jax.ShapeDtypeStruct((E, 8, 2, 2 * wide), BF),
        jax.ShapeDtypeStruct((E, ROWS, 4, wide), BF),
    )

    def body(tok, inb, outb, dgain, dbias, dw, uw, ugain, ubias, ow):
        held = pl.pallas_call(
            functools.partial(kernel, n_lat, n_lon),
            out_shape=outs,
            in_specs=[hbm] * 10,
            out_specs=(vmem, vmem),
            scratch_shapes=[
                pltpu.SMEM((n_lat + 1,), jnp.int32),
                pltpu.SMEM((n_lat + 1,), jnp.int32),
                pltpu.VMEM((4 * C,), F32),
                pltpu.VMEM((4 * C,), F32),
                pltpu.VMEM((C,), F32),
                pltpu.VMEM((C,), F32),
                pltpu.VMEM((E, ROWS, 4, wide), BF),
                pltpu.VMEM((4 * C, 2 * C), BF),
                pltpu.VMEM((2 * C, 4 * C), BF),
                pltpu.VMEM((C, C), BF),
                pltpu.VMEM((2, 160, wide), BF),
                pltpu.VMEM((2, 80, wide), BF),
                pltpu.VMEM((4, 16, wide), BF),
                pltpu.VMEM((4, 16, wide), BF),
                pltpu.VMEM((4, 16, wide), BF),
                pltpu.VMEM((16, wide), BF),
                pltpu.VMEM((16, wide), BF),
                pltpu.VMEM((16, wide), BF),
                pltpu.VMEM((16, wide), BF),
                pltpu.VMEM((4, AR, wide), BF),
                pltpu.VMEM((4, BR, wide), BF),
                pltpu.VMEM((4 * AR, 1024), BF),
                pltpu.VMEM((4 * AR, 1024), BF),
                pltpu.VMEM((4 * BR, 1024), BF),
                pltpu.VMEM((4 * BR, 1024), BF),
                pltpu.VMEM((1024, 384), BF),
                pltpu.VMEM((1024, 384), BF),
                pltpu.VMEM((2, 384, 256), BF),
                pltpu.VMEM((2, 768, 256), BF),
                pltpu.VMEM((2, 384, 256), BF),
                pltpu.VMEM((384, 384), BF),
                pltpu.VMEM((4 * AR, 768), BF),
                pltpu.VMEM((4 * BR, 768), BF),
                pltpu.VMEM((2 * AR + 2 * BR, wide), BF),
                pltpu.VMEM((2 * BR, wide), BF),
                pltpu.VMEM((176, wide), BF),
                pltpu.VMEM((64, wide), BF),
                pltpu.VMEM((4 * 176, 384), BF),
                pltpu.VMEM((4 * 64, 384), BF),
                pltpu.VMEM((240, wide), BF),
                pltpu.VMEM((56, wide), BF),
                pltpu.SemaphoreType.REGULAR,
                pltpu.SemaphoreType.DMA((10,)),
                pltpu.SemaphoreType.DMA((10 + 2 * PIECES,)),
                pltpu.SemaphoreType.DMA((10 + 2 * PIECES,)),
            ],
            compiler_params=pltpu.CompilerParams(
                collective_id=0, has_side_effects=True, vmem_limit_bytes=40000000
            ),
        )(*[pltpu.with_memory_space_constraint(v, pltpu.HBM) for v in (tok, inb, outb, dgain, dbias, dw, uw, ugain, ubias, ow)])
        return pl.pallas_call(
            copy_out,
            out_shape=outs,
            in_specs=[vmem, vmem],
            out_specs=(hbm, hbm),
            scratch_shapes=[pltpu.SemaphoreType.DMA((2,))],
            compiler_params=pltpu.CompilerParams(vmem_limit_bytes=4000000),
        )(*held)

    return jax.shard_map(
        body,
        mesh=mesh,
        in_specs=(P(None, "lat", "lon", None), P(), P(), P(), P(), P(), P(), P(), P(), P()),
        out_specs=(P(None, "lat", "lon", None), P(None, "lat", "lon", None)),
        check_vma=False,
    )
```
